32 devices in a mesh: outer: 4 (over z), inner: 8 (over y, x, core).
Axes of the slice: x: 2, y: 2, z: 4, core: 2. Of those that a mesh axis runs over, the one named last changes fastest.
Arguments:
- query_proj: bfloat16 [2048, 8192], P(('outer', 'inner')), may hold values from -8 to 8
- key_proj: bfloat16 [2048, 512], P(('outer', 'inner')), may hold values from -8 to 8
- value_proj: bfloat16 [2048, 512], P(('outer', 'inner')), may hold values from -6 to 6
- positions: int32 [2048], P(('outer', 'inner')), may hold values from 0 to 2047, each once
Outputs:
- attended: bfloat16 [2048, 8192], P(('outer', 'inner'))
The draws below stay inside these ranges and needn't reach their ends.
Inputs may be any that keep to these rules, and one draw needn't show every extreme that they name: `positions`: each position from 0 to 2047 appears exactly once.
All inputs are finite; a program needn't handle non-finite values.
Results may differ from the reference program's by a relative error of at most 0.005.
Values may be sent and summed in bfloat16 or wider, within the bound.
A program may use at most 64 MiB of HBM per device.

```python
import math
import jax
import jax.numpy as jnp
from jax import lax

HEADS = 64
KV_HEADS = 4
HEAD_WIDTH = 128
TOKENS = 2048


def draw_query_proj(key, part):
    shape_rows = TOKENS
    width = HEADS * HEAD_WIDTH
    sub_key = jax.random.fold_in(key, 1)
    base = 1.4 * jax.random.normal(sub_key, (shape_rows, width), jnp.float32)
    return jnp.clip(base, -8.0, 8.0).astype(jnp.bfloat16)


def draw_key_proj(key, part):
    shape_rows = TOKENS
    width = KV_HEADS * HEAD_WIDTH
    sub_key = jax.random.fold_in(key, 2)
    base = 1.4 * jax.random.normal(sub_key, (shape_rows, width), jnp.float32)
    return jnp.clip(base, -8.0, 8.0).astype(jnp.bfloat16)


def block_levels(stream_key, shape, shards, low, high):
    factor_of, own = 1.0, jax.random.fold_in(stream_key, 6)
    for axis_at, blocks in shards:
        heights = jnp.exp(jax.random.uniform(jax.random.fold_in(own, axis_at), (blocks,), jnp.float32, low / len(shards), high / len(shards)))
        factor_of = factor_of * jnp.repeat(heights, shape[axis_at] // blocks).reshape([-1 if axis == axis_at else 1 for axis in range(len(shape))])
    return factor_of


def gaussian(key, dims, scale, bound, shards=(), kind=jnp.bfloat16):
    array = scale * jax.random.normal(key, dims, jnp.float32)
    if shards:
        array = array * block_levels(key, dims, shards, -0.22, 0.18)
    return jnp.clip(array, -bound, bound).astype(kind)


def setup_inputs(seed: int = 0) -> dict:
    key_of = jax.random.split(jax.random.key(seed), 5)
    return {
        "query_proj": draw_query_proj(jax.random.fold_in(key_of[4], 71), 0),
        "key_proj": draw_key_proj(jax.random.fold_in(key_of[4], 71), 0),
        "value_proj": gaussian(key_of[2], (TOKENS, KV_HEADS * HEAD_WIDTH), 1.0, 6.0, ((0, 32),)),
        "positions": jax.random.permutation(key_of[3], TOKENS).astype(jnp.int32),
    }


def reference(query_proj, key_proj, value_proj, positions):
    all_tokens = query_proj.shape[0]
    group_size = HEADS // KV_HEADS
    scaling = 1.0 / math.sqrt(HEAD_WIDTH)
    query_view = query_proj.reshape(all_tokens, KV_HEADS, group_size, HEAD_WIDTH)
    key_heads = key_proj.reshape(all_tokens, KV_HEADS, HEAD_WIDTH).transpose(1, 0, 2).astype(jnp.float32)
    value_heads = value_proj.reshape(all_tokens, KV_HEADS, HEAD_WIDTH).transpose(1, 0, 2).astype(jnp.float32)
    block_rows = math.gcd(all_tokens, 512)
    block_count = all_tokens // block_rows

    def one_block(block_index):
        first_row = (block_index * block_rows).astype(jnp.int32)
        query_block = lax.dynamic_slice_in_dim(query_view, first_row, block_rows, 0).astype(jnp.float32)
        query_pos = lax.dynamic_slice_in_dim(positions, first_row, block_rows, 0)
        visible = positions[None, :] <= query_pos[:, None]

        def one_head(operands):
            query_head, key_head, value_head = operands
            scores = jnp.einsum('qgd,kd->gqk', query_head, key_head) * scaling
            row_top = lax.optimization_barrier(jnp.max(jnp.where(visible[None], scores, -1e+30), axis=2))
            softmax_weights = jnp.where(visible[None], jnp.exp(scores - row_top[:, :, None]), 0.0)
            row_total_sum = lax.optimization_barrier(jnp.sum(softmax_weights, axis=2))
            rounded = softmax_weights.astype(jnp.bfloat16).astype(jnp.float32)
            weighted = jnp.einsum('gqk,kd->gqd', rounded, value_head)
            return weighted / row_total_sum[:, :, None]
        outputs = lax.map(one_head, (query_block.transpose(1, 0, 2, 3), key_heads, value_heads))
        return outputs.transpose(2, 0, 1, 3).reshape(block_rows, HEADS * HEAD_WIDTH).astype(jnp.bfloat16)
    blocks = lax.map(one_block, jnp.arange(block_count, dtype=jnp.int32))
    return blocks.reshape(all_tokens, HEADS * HEAD_WIDTH)
```

```python
import functools
import math

import jax
import jax.numpy as jnp
from jax import lax
from jax.experimental import pallas as pl
from jax.experimental.pallas import tpu as pltpu
from jax.sharding import PartitionSpec as P

HEAD_WIDTH = 128
HIDDEN = -1e30


def kernel(sizes, q_ref, k_ref, v_ref, pos_ref, out_ref, buf, pbuf, mask, top, acc,
           copy_sem, recv_sem, send_sem):
    nz, ny, nx, rows, heads_kv, group = sizes
    d = HEAD_WIDTH
    half_heads = heads_kv // 2
    wide = half_heads * d
    chips = ny * nx
    slots = 2 * chips
    keys = slots * rows
    z = lax.axis_index("outer")
    inner = lax.axis_index("inner")
    core = lax.rem(inner, 2)
    x = lax.rem(inner // 2, nx)
    y = inner // (2 * nx)

    def dev(dz=0, dy=0, dx=0, dc=0):
        zz = lax.rem(z + dz, nz)
        yy = lax.rem(y + dy, ny)
        xx = lax.rem(x + dx, nx)
        cc = lax.rem(core + dc, 2)
        return (zz, (yy * nx + xx) * 2 + cc)

    def slot(dx, dy, dc):
        return (dc * ny + dy) * nx + dx

    local = []
    for half in range(2):
        cols = pl.ds(half * wide, wide)
        for part, ref in enumerate((k_ref, v_ref)):
            local.append(pltpu.make_async_copy(
                ref.at[:, cols], buf.at[0, half, 0, :, pl.ds(part * wide, wide)],
                copy_sem.at[2 * half + part]))
    local.append(pltpu.make_async_copy(pos_ref, pbuf.at[0, 0], copy_sem.at[4]))
    for c in local:
        c.start()

    barrier = pltpu.get_barrier_semaphore()
    peers = [dict(dz=i) for i in range(1, nz)] + [dict(dy=i) for i in range(1, ny)]
    peers += [dict(dx=i) for i in range(1, nx)] + [dict(dc=1)]
    for peer in peers:
        pl.semaphore_signal(barrier, inc=1, device_id=dev(**peer),
                            device_id_type=pl.DeviceIdType.MESH)
    pl.semaphore_wait(barrier, len(peers))
    for c in local:
        c.wait()

    sent = []

    def ref_of(s, kind, sl):
        return pbuf.at[s, sl] if kind == 2 else buf.at[s, kind, sl]

    def send(src, dst, to):
        n = len(sent)
        c = pltpu.make_async_remote_copy(
            src_ref=ref_of(*src), dst_ref=ref_of(*dst), send_sem=send_sem.at[n],
            recv_sem=recv_sem.at[dst[0], dst[1], dst[2]], device_id=dev(**to),
            device_id_type=pl.DeviceIdType.MESH)
        c.start()
        sent.append(c)

    def arrived(s, kind, sl):
        r = ref_of(s, kind, sl)
        pltpu.make_async_remote_copy(
            src_ref=r, dst_ref=r, send_sem=send_sem.at[0],
            recv_sem=recv_sem.at[s, kind, sl], device_id=dev(dc=1),
            device_id_type=pl.DeviceIdType.MESH).wait_recv()

    KINDS = (2, 0, 1)

    def issue_column(s):
        for kind in KINDS:
            if s:
                arrived(s, kind, 0)
            src = (s, kind, 0)
            order = ("x", "y") if kind != 1 else ("y", "x")
            for axis in order:
                if axis == "x":
                    for dx in range(1, nx):
                        send(src, (s, kind, slot(dx, 0, 0)), dict(dx=dx))
                else:
                    for dy in range(1, ny):
                        send(src, (s, kind, slot(0, dy, 0)), dict(dy=dy))
            send(src, (s, kind, slot(0, 0, 1)), dict(dc=1))

    def to_sibling(s, kind, dx, dy):
        send((s, kind, slot(dx, dy, 0)), (s, kind, slot(dx, dy, 1)), dict(dc=1))

    def relay(s):
        for kind in (2, 0):
            for dx in range(1, nx):
                here = slot(dx, 0, 0)
                arrived(s, kind, here)
                for dy in range(1, ny):
                    send((s, kind, here), (s, kind, slot(dx, dy, 0)), dict(dy=dy))
                to_sibling(s, kind, dx, 0)
        for dy in range(1, ny):
            here = slot(0, dy, 0)
            arrived(s, 1, here)
            for dx in range(1, nx):
                send((s, 1, here), (s, 1, slot(dx, dy, 0)), dict(dx=dx))
            to_sibling(s, 1, 0, dy)
        for dx in range(1, nx):
            arrived(s, 1, slot(dx, 0, 0))
            to_sibling(s, 1, dx, 0)
        for kind in (2, 0):
            for dy in range(1, ny):
                arrived(s, kind, slot(0, dy, 0))
                to_sibling(s, kind, 0, dy)

    def gather_rest(s):
        for kind in KINDS:
            for dy in range(1, ny):
                for dx in range(1, nx):
                    arrived(s, kind, slot(dx, dy, 0))
                    to_sibling(s, kind, dx, dy)
        for kind in KINDS:
            for sl in range(chips, slots):
                arrived(s, kind, sl)

    def build_mask(s):
        mine = jnp.concatenate([pos_ref[...], pos_ref[...]], axis=1)
        mine = jnp.broadcast_to(mine.astype(jnp.float32), (rows, 2 * rows))
        for sl in range(slots):
            theirs = jnp.broadcast_to(pbuf[s, sl].astype(jnp.float32), (2 * rows, rows)).T
            mask[sl * rows:(sl + 1) * rows, :] = jnp.where(
                theirs > mine, HIDDEN, 0.0).astype(jnp.bfloat16)

    eye = (lax.broadcasted_iota(jnp.int32, (rows, 2 * rows), 0)
           == lax.broadcasted_iota(jnp.int32, (rows, 2 * rows), 1)).astype(jnp.bfloat16)
    scale = math.log2(math.e) / math.sqrt(d)
    per_tile = math.gcd(4, group)
    tile = per_tile * rows
    tiles = group // per_tile

    def one_tile(s, half, hh, t):
        head = half * half_heads + hh
        first = head * group + t * per_tile
        at = pl.multiple_of(first * rows, tile)
        query = jnp.concatenate(
            [jnp.concatenate(
                [q_ref[:, pl.ds(pl.multiple_of((first + j) * d, d), d)], eye], axis=1)
             for j in range(per_tile)], axis=0)
        k_tile = buf[s, half, :, :, hh * d:(hh + 1) * d].reshape(keys, d)
        v_tile = buf[s, half, :, :, wide + hh * d:wide + (hh + 1) * d].reshape(keys, d)
        k_wide = jnp.concatenate([k_tile, mask[...]], axis=1)
        v_wide = jnp.concatenate([v_tile, jnp.ones((keys, d), jnp.bfloat16)], axis=1)
        scores = lax.dot_general(query, k_wide, (((1,), (1,)), ((), ())),
                                 preferred_element_type=jnp.float32)
        block_top = jnp.max(scores, axis=1, keepdims=True)
        window = pl.ds(at, tile)
        if s == 0:
            new_top = block_top
        else:
            old_top = top[window, :1]
            new_top = jnp.maximum(old_top, block_top)
            rescale = jnp.exp2((old_top - new_top) * scale)
        weights = jnp.exp2((scores - new_top) * scale).astype(jnp.bfloat16)
        got = lax.dot_general(weights, v_wide, (((1,), (0,)), ((), ())),
                              preferred_element_type=jnp.float32)
        if s:
            got = acc[window, :] * rescale + got
        if s < nz - 1:
            acc[window, :] = got
            top[window, :] = jnp.broadcast_to(new_top, (tile, d))
        else:
            result = (got[:, :d] / got[:, d:]).astype(jnp.bfloat16)
            for j in range(per_tile):
                out_ref[:, pl.ds(pl.multiple_of((first + j) * d, d), d)] = (
                    result[j * rows:(j + 1) * rows, :])

    def compute(s, half):
        for hh in range(half_heads):
            @pl.loop(0, tiles // 2)
            def _(t):
                for u in range(2):
                    one_tile(s, half, hh, t * 2 + u)

    for dz in range(1, nz):
        for kind in KINDS:
            send((0, kind, 0), (dz, kind, 0), dict(dz=dz))
            if dz == 1:
                pass
    issue_column(0)
    relay(0)
    issue_column(1)
    for s in range(nz):
        gather_rest(s)
        build_mask(s)
        compute(s, 0)
        if s + 1 < nz:
            relay(s + 1)
        if s + 2 < nz:
            issue_column(s + 2)
        compute(s, 1)
    for c in sent:
        c.wait_send()


def body(query_proj, key_proj, value_proj, positions):
    rows, width = query_proj.shape
    d = HEAD_WIDTH
    heads_kv = key_proj.shape[1] // d
    group = width // d // heads_kv
    nz = lax.axis_size("outer")
    inner = lax.axis_size("inner")
    nx = 2
    ny = inner // 4
    slots = inner
    sizes = (nz, ny, nx, rows, heads_kv, group)
    wide = heads_kv // 2 * d
    copies = 3 * (nz - 1) + nz * (3 * (nx - 1 + ny - 1 + slots // 2) + 3 * (nx - 1) * (ny - 1))
    return pl.pallas_call(
        functools.partial(kernel, sizes),
        out_shape=jax.ShapeDtypeStruct((rows, width), jnp.bfloat16),
        in_specs=[pl.BlockSpec(memory_space=pltpu.VMEM), pl.BlockSpec(memory_space=pl.ANY),
                  pl.BlockSpec(memory_space=pl.ANY), pl.BlockSpec(memory_space=pltpu.VMEM)],
        out_specs=pl.BlockSpec(memory_space=pltpu.VMEM),
        scratch_shapes=[
            pltpu.VMEM((nz, 2, slots, rows, 2 * wide), jnp.bfloat16),
            pltpu.VMEM((nz, slots, 1, rows), jnp.int32),
            pltpu.VMEM((slots * rows, d), jnp.bfloat16),
            pltpu.VMEM((width // d * rows, d), jnp.float32),
            pltpu.VMEM((width // d * rows, 2 * d), jnp.float32),
            pltpu.SemaphoreType.DMA((5,)),
            pltpu.SemaphoreType.DMA((nz, 3, slots)),
            pltpu.SemaphoreType.DMA((copies,)),
        ],
        compiler_params=pltpu.CompilerParams(
            collective_id=0, has_side_effects=True, vmem_limit_bytes=56 * 1024 * 1024),
    )(query_proj, key_proj, value_proj, positions.reshape(1, rows))


def solution(mesh):
    return jax.shard_map(
        body,
        mesh=mesh,
        in_specs=(
            P(("outer", "inner"), None),
            P(("outer", "inner"), None),
            P(("outer", "inner"), None),
            P(("outer", "inner")),
        ),
        out_specs=P(("outer", "inner"), None),
        check_vma=False,
    )
```

```python
import functools
import math

import jax
import jax.numpy as jnp
from jax import lax
from jax.experimental import pallas as pl
from jax.experimental.pallas import tpu as pltpu
from jax.sharding import PartitionSpec as P

HEAD_WIDTH = 128
HIDDEN = -1e30


def kernel(sizes, q_ref, k_ref, v_ref, pos_ref, out_ref, buf, pbuf, mask, top, acc,
           q_buf, copy_sem, recv_sem, send_sem):
    nz, ny, nx, rows, heads_kv, group = sizes
    d = HEAD_WIDTH
    half_heads = heads_kv // 2
    wide = half_heads * d
    chips = ny * nx
    slots = 2 * chips
    keys = slots * rows
    z = lax.axis_index("outer")
    inner = lax.axis_index("inner")
    core = lax.rem(inner, 2)
    x = lax.rem(inner // 2, nx)
    y = inner // (2 * nx)

    def dev(dz=0, dy=0, dx=0, dc=0):
        zz = lax.rem(z + dz, nz)
        yy = lax.rem(y + dy, ny)
        xx = lax.rem(x + dx, nx)
        cc = lax.rem(core + dc, 2)
        return (zz, (yy * nx + xx) * 2 + cc)

    def slot(dx, dy, dc):
        return (dc * ny + dy) * nx + dx

    query_copy = pltpu.make_async_copy(q_ref, q_buf, copy_sem.at[5])
    local = []
    for half in range(2):
        cols = pl.ds(half * wide, wide)
        for part, ref in enumerate((k_ref, v_ref)):
            local.append(pltpu.make_async_copy(
                ref.at[:, cols], buf.at[0, half, 0, :, pl.ds(part * wide, wide)],
                copy_sem.at[2 * half + part]))
    local.append(pltpu.make_async_copy(pos_ref, pbuf.at[0, 0], copy_sem.at[4]))
    for c in local:
        c.start()

    query_copy.start()
    barrier = pltpu.get_barrier_semaphore()
    peers = [dict(dz=i) for i in sorted({1 % nz, nz - 1} - {0})] + [dict(dy=i) for i in range(1, ny)]
    peers += [dict(dx=i) for i in range(1, nx)] + [dict(dc=1)]
    for peer in peers:
        pl.semaphore_signal(barrier, inc=1, device_id=dev(**peer),
                            device_id_type=pl.DeviceIdType.MESH)
    pl.semaphore_wait(barrier, len(peers))
    for c in local:
        c.wait()

    sent = []

    def ref_of(s, kind, sl):
        return pbuf.at[s, sl] if kind == 2 else buf.at[s, kind, sl]

    def send(src, dst, to):
        n = len(sent)
        c = pltpu.make_async_remote_copy(
            src_ref=ref_of(*src), dst_ref=ref_of(*dst), send_sem=send_sem.at[n],
            recv_sem=recv_sem.at[dst[0], dst[1], dst[2]], device_id=dev(**to),
            device_id_type=pl.DeviceIdType.MESH)
        c.start()
        sent.append(c)

    def arrived(s, kind, sl):
        r = ref_of(s, kind, sl)
        pltpu.make_async_remote_copy(
            src_ref=r, dst_ref=r, send_sem=send_sem.at[0],
            recv_sem=recv_sem.at[s, kind, sl], device_id=dev(dc=1),
            device_id_type=pl.DeviceIdType.MESH).wait_recv()

    KINDS = (2, 0, 1)

    def issue_column(s):
        for kind in KINDS:
            if s:
                arrived(s, kind, 0)
            src = (s, kind, 0)
            if s + 1 < nz:
                send(src, (s + 1, kind, 0), dict(dz=1))
            order = ("x", "y") if kind != 1 else ("y", "x")
            for axis in order:
                if axis == "x":
                    for dx in range(1, nx):
                        send(src, (s, kind, slot(dx, 0, 0)), dict(dx=dx))
                else:
                    for dy in range(1, ny):
                        send(src, (s, kind, slot(0, dy, 0)), dict(dy=dy))
            send(src, (s, kind, slot(0, 0, 1)), dict(dc=1))

    def to_sibling(s, kind, dx, dy):
        send((s, kind, slot(dx, dy, 0)), (s, kind, slot(dx, dy, 1)), dict(dc=1))

    def relay(s):
        for kind in (2, 0):
            for dx in range(1, nx):
                here = slot(dx, 0, 0)
                arrived(s, kind, here)
                for dy in range(1, ny):
                    send((s, kind, here), (s, kind, slot(dx, dy, 0)), dict(dy=dy))
                to_sibling(s, kind, dx, 0)
        for dy in range(1, ny):
            here = slot(0, dy, 0)
            arrived(s, 1, here)
            for dx in range(1, nx):
                send((s, 1, here), (s, 1, slot(dx, dy, 0)), dict(dx=dx))
            to_sibling(s, 1, 0, dy)
        for dx in range(1, nx):
            arrived(s, 1, slot(dx, 0, 0))
            to_sibling(s, 1, dx, 0)
        for kind in (2, 0):
            for dy in range(1, ny):
                arrived(s, kind, slot(0, dy, 0))
                to_sibling(s, kind, 0, dy)

    def gather_rest(s):
        for kind in KINDS:
            for dy in range(1, ny):
                for dx in range(1, nx):
                    arrived(s, kind, slot(dx, dy, 0))
                    to_sibling(s, kind, dx, dy)
        for kind in KINDS:
            for sl in range(chips, slots):
                arrived(s, kind, sl)

    def build_mask(s):
        mine = jnp.concatenate([pos_ref[...], pos_ref[...]], axis=1)
        mine = jnp.broadcast_to(mine.astype(jnp.float32), (rows, 2 * rows))
        for sl in range(slots):
            theirs = jnp.broadcast_to(pbuf[s, sl].astype(jnp.float32), (2 * rows, rows)).T
            mask[sl * rows:(sl + 1) * rows, :] = jnp.where(
                theirs > mine, HIDDEN, 0.0).astype(jnp.bfloat16)

    eye = (lax.broadcasted_iota(jnp.int32, (rows, 2 * rows), 0)
           == lax.broadcasted_iota(jnp.int32, (rows, 2 * rows), 1)).astype(jnp.bfloat16)
    scale = math.log2(math.e) / math.sqrt(d)
    per_tile = math.gcd(8, group)
    tile = per_tile * rows
    tiles = group // per_tile

    ones = jnp.ones((keys, d), jnp.bfloat16)

    def compute(s, half):
        @pl.loop(0, half_heads)
        def _(hh):
            head = half * half_heads + hh
            k_cols = pl.ds(pl.multiple_of(hh * d, d), d)
            v_cols = pl.ds(pl.multiple_of(wide + hh * d, d), d)
            k_wide = jnp.concatenate([buf[s, half, :, :, k_cols].reshape(keys, d), mask[...]],
                                     axis=1)
            v_wide = jnp.concatenate([buf[s, half, :, :, v_cols].reshape(keys, d), ones], axis=1)

            def columns(t, j):
                return pl.ds(pl.multiple_of((head * group + t * per_tile + j) * d, d), d)

            def score(t):
                query = jnp.concatenate(
                    [jnp.concatenate([q_buf[:, columns(t, j)], eye], axis=1)
                     for j in range(per_tile)], axis=0)
                return lax.dot_general(query, k_wide, (((1,), (1,)), ((), ())),
                                       preferred_element_type=jnp.float32)

            def fold(t, scores):
                window = slice(t * tile, (t + 1) * tile)
                new_top = jnp.broadcast_to(jnp.max(scores, axis=1, keepdims=True), (tile, d))
                if s:
                    old_top = top[head, window, :]
                    new_top = jnp.maximum(old_top, new_top)
                    rescale = jnp.exp2((old_top - new_top) * scale)
                weights = jnp.exp2((scores - jnp.concatenate([new_top] * (keys // d), axis=1)) * scale).astype(jnp.bfloat16)
                got = lax.dot_general(weights, v_wide, (((1,), (0,)), ((), ())),
                                      preferred_element_type=jnp.float32)
                if s:
                    got = acc[head, window, :] * jnp.concatenate([rescale, rescale], axis=1) + got
                if s < nz - 1:
                    acc[head, window, :] = got
                    top[head, window, :] = new_top
                else:
                    result = (got[:, :d] / got[:, d:]).astype(jnp.bfloat16)
                    for j in range(per_tile):
                        out_ref[:, columns(t, j)] = result[j * rows:(j + 1) * rows, :]

            held = score(0)
            for t in range(tiles):
                following = score(t + 1) if t + 1 < tiles else None
                fold(t, held)
                held = following

    issue_column(0)
    relay(0)
    if nz > 1:
        issue_column(1)
    gather_rest(0)
    query_copy.wait()
    for s in range(nz):
        build_mask(s)
        compute(s, 0)
        if s == 0 and nz > 2:
            issue_column(2)
        elif 0 < s < nz - 1:
            relay(s + 1)
        compute(s, 1)
        if s == 0 and nz > 1:
            relay(1)
        if s + 3 < nz:
            issue_column(s + 3)
        if s + 1 < nz:
            gather_rest(s + 1)
    for c in sent:
        c.wait_send()


def body(query_proj, key_proj, value_proj, positions):
    rows, width = query_proj.shape
    d = HEAD_WIDTH
    heads_kv = key_proj.shape[1] // d
    group = width // d // heads_kv
    nz = lax.axis_size("outer")
    inner = lax.axis_size("inner")
    nx = 2
    ny = inner // 4
    slots = inner
    sizes = (nz, ny, nx, rows, heads_kv, group)
    wide = heads_kv // 2 * d
    copies = 3 * (nz - 1) + nz * (3 * (nx - 1 + ny - 1 + slots // 2) + 3 * (nx - 1) * (ny - 1))
    return pl.pallas_call(
        functools.partial(kernel, sizes),
        out_shape=jax.ShapeDtypeStruct((rows, width), jnp.bfloat16),
        in_specs=[pl.BlockSpec(memory_space=pl.ANY), pl.BlockSpec(memory_space=pl.ANY),
                  pl.BlockSpec(memory_space=pl.ANY), pl.BlockSpec(memory_space=pltpu.VMEM)],
        out_specs=pl.BlockSpec(memory_space=pltpu.VMEM),
        scratch_shapes=[
            pltpu.VMEM((nz, 2, slots, rows, 2 * wide), jnp.bfloat16),
            pltpu.VMEM((nz, slots, 1, rows), jnp.int32),
            pltpu.VMEM((slots * rows, d), jnp.bfloat16),
            pltpu.VMEM((heads_kv, group * rows, d), jnp.float32),
            pltpu.VMEM((heads_kv, group * rows, 2 * d), jnp.float32),
            pltpu.VMEM((rows, width), jnp.bfloat16),
            pltpu.SemaphoreType.DMA((6,)),
            pltpu.SemaphoreType.DMA((nz, 3, slots)),
            pltpu.SemaphoreType.DMA((copies,)),
        ],
        compiler_params=pltpu.CompilerParams(
            collective_id=0, has_side_effects=True, vmem_limit_bytes=44 * 1024 * 1024),
    )(query_proj, key_proj, value_proj, positions.reshape(1, rows))


def solution(mesh):
    return jax.shard_map(
        body,
        mesh=mesh,
        in_specs=(
            P(("outer", "inner"), None),
            P(("outer", "inner"), None),
            P(("outer", "inner"), None),
            P(("outer", "inner")),
        ),
        out_specs=P(("outer", "inner"), None),
        check_vma=False,
    )
```
